32 devices in a mesh: dp: 8 (over z, y), tensor: 4 (over x, core).
Axes of the slice: x: 2, y: 2, z: 4, core: 2. Of those that a mesh axis runs over, the one named last changes fastest.
Arguments:
- grads: bfloat16 [8, 2, 4096, 1024], P('dp', None, None, 'tensor'), may hold values from -480 to 480
- master: float32 [2, 4096, 1024], P(None, 'dp', 'tensor'), may hold values from -0.09375 to 0.09375
- moment: float32 [2, 4096, 1024], P(None, 'dp', 'tensor'), may hold values from -0.06 to 0.06
- v_heads: float32 [8], P('tensor'), may hold values from 0.0001 to 0.001
- v_neurons: float32 [1024], P('tensor'), may hold values from 0.0001 to 0.001
Outputs:
- params: bfloat16 [2, 4096, 1024], P(None, None, 'tensor')
- new_master: float32 [2, 4096, 1024], P(None, 'dp', 'tensor')
- new_moment: float32 [2, 4096, 1024], P(None, 'dp', 'tensor')
- new_heads: float32 [8], P('tensor')
- new_neurons: float32 [1024], P('tensor')
The draws below stay inside these ranges and needn't reach their ends.
All inputs are finite; a program needn't handle non-finite values.
Results may differ from the reference program's by a relative error of at most 0.001.
Values may be sent and summed in bfloat16 or wider, within the bound.
A program may use at most 64 MiB of HBM per device.

```python
import math
import jax
import jax.numpy as jnp
from jax import lax

DIN = 4096
KVH = 8
HEAD = 128
STEP = 2
N_DP = 8


def draw_grads(key, part):
    columns = KVH * HEAD
    keys = jax.random.split(key, 3)
    row_rand = jnp.exp(jax.random.uniform(keys[0], (DIN,), jnp.float32, 0.0, math.log(10.0)))
    rows = jnp.arange(DIN, dtype=jnp.float32) / DIN
    row_scale = row_rand * (1.0 + 2.0 * rows)
    col_scale = 1.0 + 2.0 * jnp.arange(columns, dtype=jnp.float32) / columns
    order = jax.random.permutation(keys[1], N_DP)
    row_block = jnp.arange(DIN) // (DIN // N_DP)
    spike = jnp.where(row_block[None, :] == order[:, None], 4.0, 1.0)
    shape = (N_DP, 2, DIN, columns)
    base = jnp.clip(jax.random.normal(keys[2], shape, jnp.float32), -4.0, 4.0)
    values = base * spike[:, None, :, None] * row_scale[None, None, :, None] * col_scale[None, None, None, :]
    values = jnp.clip(values, -480.0, 480.0)
    return values.astype(jnp.bfloat16)


def level_of(stream_key, extent, shards, smallest, top_value):
    loudness = 1.0
    for dim, parts in shards:
        steps = jax.random.uniform(jax.random.fold_in(jax.random.fold_in(stream_key, 6), dim), (parts,), jnp.float32, smallest / len(shards), top_value / len(shards))
        loudness = loudness * jnp.repeat(jnp.exp(steps), extent[dim] // parts).reshape((-1,) + (1,) * (len(extent) - 1 - dim))
    return loudness


def bell_draw(own_key, dims, width, limit, shards=(), held_as=jnp.bfloat16):
    result = jax.random.normal(own_key, dims, jnp.float32) * width
    if len(shards) > 0:
        result = level_of(own_key, dims, shards, -0.22, 0.18) * result
    return jnp.clip(result, min=-limit, max=limit).astype(held_as)


def setup_inputs(seed: int = 0) -> dict:
    streams_of = jax.random.split(jax.random.key(seed), 6)
    return {
        "grads": draw_grads(jax.random.fold_in(streams_of[5], 71), 0),
        "master": bell_draw(streams_of[1], (2, DIN, KVH * HEAD), DIN ** -0.5, 0.09375, ((1, 8), (2, 4)), jnp.float32),
        "moment": bell_draw(streams_of[2], (2, DIN, KVH * HEAD), 0.01, 0.06, ((1, 8), (2, 4)), jnp.float32),
        "v_heads": jnp.clip(jnp.exp(math.log(0.001) - 2.3025852 * jax.random.uniform(streams_of[3], (KVH,), jnp.float32) ** level_of(streams_of[3], (KVH,), ((0, 4),), -0.2, 0.2)), 0.0001, 0.001),
        "v_neurons": jnp.clip(jnp.exp(math.log(0.001) - 2.3025852 * jax.random.uniform(streams_of[4], (KVH * HEAD,), jnp.float32) ** level_of(streams_of[4], (KVH * HEAD,), ((0, 4),), -0.2, 0.2)), 0.0001, 0.001),
    }


def reference(grads, master, moment, v_heads, v_neurons):

    def add_replica(index, total):
        return total + lax.dynamic_index_in_dim(grads, index, 0, keepdims=False).astype(jnp.float32)
    summed = lax.fori_loop(0, N_DP, add_replica, jnp.zeros(grads.shape[1:], jnp.float32))
    gradient = summed / N_DP
    keys = gradient[0].reshape(DIN, KVH, HEAD)
    head_sq = lax.optimization_barrier(jnp.sum(keys * keys, axis=(0, 2)))
    neuron_sq = lax.optimization_barrier(jnp.sum(gradient[1] * gradient[1], axis=0))
    total = jnp.sum(head_sq) + jnp.sum(neuron_sq)
    clip = jnp.minimum(1.0, 256.0 / (jnp.sqrt(total) + 1e-06))
    new_moment = 0.9 * moment + 0.1 * clip * gradient
    new_heads = 0.95 * v_heads + 0.05 * clip * clip * head_sq / (DIN * HEAD)
    new_neurons = 0.95 * v_neurons + 0.05 * clip * clip * neuron_sq / DIN
    second_fix = 1.0 - 0.95 ** STEP
    first_fix = 1.0 - 0.9 ** STEP
    key_denom = jnp.repeat(jnp.sqrt(new_heads / second_fix) + 1e-08, HEAD)
    value_denom = jnp.sqrt(new_neurons / second_fix) + 1e-08
    denom = jnp.stack([key_denom, value_denom])
    update = new_moment / first_fix / denom[:, None, :]
    new_master = master - 0.01 * (update + 0.1 * master)
    params = new_master.astype(jnp.bfloat16)
    return (params, new_master, new_moment, new_heads, new_neurons)
```

```python
import functools

import jax
import jax.numpy as jnp
from jax import lax
from jax.experimental import pallas as pl
from jax.experimental.pallas import tpu as pltpu
from jax.sharding import PartitionSpec as P

HEAD = 128
STEP = 2
LIMIT = 480.0
MESH = pl.DeviceIdType.MESH
TILE = 32


def encode(x, scale):
    z = x * scale
    return (z * jnp.abs(z) * (z * z)).astype(jnp.bfloat16)


def decode(code, scale):
    y = code.astype(jnp.float32)
    root = lax.rsqrt(lax.rsqrt(jnp.abs(y))) * (1.0 / scale)
    return jnp.where(y < 0, -root, root)


def kernel(
    A, B, T, n_rows,
    grads, master, moment, v_heads, v_neurons,
    params, new_master, new_moment, new_v,
    own, raw, part_out, up_in, down_in, gsum, mas, mom, stat, stat_in, tot, tot_in,
    own_sem, mm_sem, raw_s, raw_r, part_s, up_r, down_r, stat_s, stat_r, tot_s, tot_r,
    zup_s, zup_r, zdn_s, zdn_r, in_s, in_r,
):
    nproj, n, R, C = grads.shape
    me = lax.axis_index("dp")
    mt = lax.axis_index("tensor")
    a, b = me // B, me % B
    tile = min(TILE, R)
    scale = 2.0**31 / (LIMIT * n)

    def at_dp(i):
        return {"dp": i}

    def peer(j):
        return (b + j) % B

    barrier = pltpu.get_barrier_semaphore()
    for j in range(1, n):
        pl.semaphore_signal(barrier, inc=1, device_id=at_dp((me + j) % n), device_id_type=MESH)
    for j in range(1, T):
        pl.semaphore_signal(barrier, inc=1, device_id={"tensor": (mt + j) % T}, device_id_type=MESH)

    def own_copy(at, p):
        return pltpu.make_async_copy(grads.at[p, at * B + b], own.at[at, p], own_sem.at[at, p])

    mm = [
        pltpu.make_async_copy(master, mas, mm_sem.at[0]),
        pltpu.make_async_copy(moment, mom, mm_sem.at[1]),
    ]

    def in_order(use):
        for d in range(A - 1, 0, -1):
            @pl.when(a + d <= A - 1)
            def _():
                use(a + d, 1)

            @pl.when(a - d >= 0)
            def _():
                use(a - d, -1)
        use(a, 0)

    def raw_copy(at, j, p):
        to = peer(j)
        return pltpu.make_async_remote_copy(
            src_ref=grads.at[p, at * B + to], dst_ref=raw.at[at, j - 1, p],
            send_sem=raw_s.at[at, j - 1, p], recv_sem=raw_r.at[at, j - 1, p],
            device_id=at_dp(a * B + to), device_id_type=MESH,
        )

    def start_own(at, side):
        for p in range(nproj):
            own_copy(at, p).start()

    def start_raw(at, side):
        for p in range(nproj):
            for j in range(1, B):
                raw_copy(at, j, p).start()

    in_order(start_own)
    for c in mm:
        c.start()
    pl.semaphore_wait(barrier, n - 1 + T - 1)
    in_order(start_raw)

    def up_copy(at, p):
        return pltpu.make_async_remote_copy(
            src_ref=part_out.at[at, p], dst_ref=up_in.at[at, p],
            send_sem=part_s.at[at, p], recv_sem=up_r.at[at, p],
            device_id=at_dp(jnp.minimum(me + B, n - 1)), device_id_type=MESH,
        )

    def down_copy(at, p):
        return pltpu.make_async_remote_copy(
            src_ref=part_out.at[at, p], dst_ref=down_in.at[at, p],
            send_sem=part_s.at[at, p], recv_sem=down_r.at[at, p],
            device_id=at_dp(jnp.maximum(me - B, 0)), device_id_type=MESH,
        )

    def local_sum(at, p, rows):
        x = own[at, p, rows].astype(jnp.float32)
        for j in range(B - 1):
            x = x + raw[at, j, p, rows].astype(jnp.float32)
        return x

    def tiles(body):
        def step(i, carry):
            body(pl.ds(pl.multiple_of(i * tile, tile), tile))
            return carry
        lax.fori_loop(0, R // tile, step, 0)

    def combine(at, side):
        for p in range(nproj):
            own_copy(at, p).wait()
            for j in range(1, B):
                raw_copy(at, j, p).wait_recv()
            if side == 0:
                tiles(lambda rows, p=p: gsum.__setitem__((p, rows), local_sum(at, p, rows)))
                for inn, copy, cond in ((up_in, up_copy, a > 0), (down_in, down_copy, a < A - 1)):
                    @pl.when(cond)
                    def _():
                        copy(at, p).wait_recv()

                        def add(rows):
                            gsum[p, rows] = gsum[p, rows] + decode(inn[at, p, rows], scale)
                        tiles(add)
                continue
            inn, copy = (up_in, up_copy) if side > 0 else (down_in, down_copy)
            first = (a == 0) if side > 0 else (a == A - 1)

            @pl.when(first)
            def _():
                def put(rows):
                    part_out[at, p, rows] = encode(local_sum(at, p, rows), scale)
                tiles(put)

            @pl.when(jnp.logical_not(first))
            def _():
                copy(at, p).wait_recv()

                def put(rows):
                    x = local_sum(at, p, rows) + decode(inn[at, p, rows], scale)
                    part_out[at, p, rows] = encode(x, scale)
                tiles(put)
            copy(at, p).start()

    in_order(combine)

    inv = 1.0 / n

    for p in range(nproj):
        def sq(i, acc):
            rows = pl.ds(pl.multiple_of(i * tile, tile), tile)
            g = gsum[p, rows] * inv
            gsum[p, rows] = g
            g = (g * g).reshape(tile // 8, 8, C)
            return acc + jnp.sum(g, axis=0)
        acc = lax.fori_loop(0, R // tile, sq, jnp.zeros((8, C), jnp.float32))
        stat[p : p + 1, :] = jnp.sum(acc, axis=0, keepdims=True)

    def stat_copy(j):
        return pltpu.make_async_remote_copy(
            src_ref=stat, dst_ref=stat_in.at[j - 1], send_sem=stat_s.at[j - 1], recv_sem=stat_r.at[j - 1],
            device_id=at_dp((me + j) % n), device_id_type=MESH,
        )

    for j in range(1, n):
        stat_copy(j).start()
    sums = stat[...]
    for j in range(1, n):
        stat_copy(j).wait_recv()
        sums = sums + stat_in[j - 1]
    tot[...] = jnp.broadcast_to(jnp.sum(sums), tot.shape)

    def tot_copy(j):
        return pltpu.make_async_remote_copy(
            src_ref=tot, dst_ref=tot_in.at[j - 1], send_sem=tot_s.at[j - 1], recv_sem=tot_r.at[j - 1],
            device_id={"tensor": (mt + j) % T}, device_id_type=MESH,
        )

    for j in range(1, T):
        tot_copy(j).start()
    total = tot[0:1, :]
    for j in range(1, T):
        tot_copy(j).wait_recv()
        total = total + tot_in[j - 1, 0:1, :]
    clip = jnp.minimum(1.0, 256.0 / (jnp.sqrt(total) + 1e-06))
    clip = jnp.concatenate([clip] * (C // HEAD), axis=1)
    heads = []
    for h in range(C // HEAD):
        head = jnp.sum(sums[0:1, h * HEAD : (h + 1) * HEAD], axis=1, keepdims=True)
        heads.append(0.95 * v_heads[h] + 0.05 * (clip * clip)[:, :HEAD] * head / (n_rows * HEAD))
    v_key = jnp.concatenate(heads, axis=1)
    v_val = 0.95 * v_neurons[...] + 0.05 * clip * clip * sums[1:2, :] / n_rows
    new_v[0:1, :] = v_key
    new_v[1:2, :] = v_val
    second_fix = 1.0 - 0.95**STEP
    first_fix = 1.0 - 0.9**STEP
    for c in mm:
        c.wait()

    def up_gather(at, p):
        return pltpu.make_async_remote_copy(
            src_ref=params.at[p, at * B + b], dst_ref=params.at[p, at * B + b],
            send_sem=zup_s.at[at, p], recv_sem=zup_r.at[at, p],
            device_id=at_dp(jnp.minimum(me + B, n - 1)), device_id_type=MESH,
        )

    def down_gather(at, p):
        return pltpu.make_async_remote_copy(
            src_ref=params.at[p, at * B + b], dst_ref=params.at[p, at * B + b],
            send_sem=zdn_s.at[at, p], recv_sem=zdn_r.at[at, p],
            device_id=at_dp(jnp.maximum(me - B, 0)), device_id_type=MESH,
        )

    def in_gather(at, j, p, col):
        return pltpu.make_async_remote_copy(
            src_ref=params.at[p, at * B + col], dst_ref=params.at[p, at * B + col],
            send_sem=in_s.at[at, j - 1, p], recv_sem=in_r.at[at, j - 1, p],
            device_id=at_dp(a * B + peer(j)), device_id_type=MESH,
        )

    for p in range(nproj):
        v = v_key if p == 0 else v_val
        rate = 1.0 / (first_fix * (jnp.sqrt(v / second_fix) + 1e-08))
        gain = 0.1 * clip

        def update(rows):
            fresh = 0.9 * mom[p, rows] + gain * gsum[p, rows]
            w = mas[p, rows]
            w = w - 0.01 * (fresh * rate + 0.1 * w)
            new_moment[p, rows] = fresh
            new_master[p, rows] = w
            params[p, me, rows] = w.astype(jnp.bfloat16)
        tiles(update)
        for j in range(1, B):
            in_gather(a, j, p, b).start()

        @pl.when(a < A - 1)
        def _():
            up_gather(a, p).start()

        @pl.when(a > 0)
        def _():
            down_gather(a, p).start()

    for d in range(1, A):
        for p in range(nproj):
            @pl.when(a - d >= 0)
            def _():
                at = a - d
                up_gather(at, p).wait_recv()

                @pl.when(a < A - 1)
                def _():
                    up_gather(at, p).start()
                for j in range(1, B):
                    in_gather(at, j, p, b).start()

            @pl.when(a + d <= A - 1)
            def _():
                at = a + d
                down_gather(at, p).wait_recv()

                @pl.when(a > 0)
                def _():
                    down_gather(at, p).start()
                for j in range(1, B):
                    in_gather(at, j, p, b).start()

    def finish(at, side):
        for p in range(nproj):
            for j in range(1, B):
                raw_copy(at, j, p).wait_send()
            if side > 0:
                up_copy(at, p).wait_send()
            elif side < 0:
                down_copy(at, p).wait_send()
            if side <= 0:
                @pl.when(a < A - 1)
                def _():
                    up_gather(at, p).wait_send()
            if side >= 0:
                @pl.when(a > 0)
                def _():
                    down_gather(at, p).wait_send()
            for j in range(1, B):
                in_gather(at, j, p, b).wait_send()
                in_gather(at, j, p, (b - j + B) % B).wait_recv()

    in_order(finish)
    for j in range(1, n):
        stat_copy(j).wait_send()
    for j in range(1, T):
        tot_copy(j).wait_send()


def inner_size(mesh):
    line = mesh.devices.reshape(mesh.shape["dp"], -1)[:, 0]
    n = len(line)
    spots = [getattr(d, "coords", None) for d in line]
    if any(s is None or len(s) < 3 for s in spots):
        return 2 if n % 2 == 0 else 1
    inner = sum(s[2] == spots[0][2] for s in spots)
    return inner if n % inner == 0 else 1


def on_device(B, grads, master, moment, v_heads, v_neurons):
    n, T = lax.axis_size("dp"), lax.axis_size("tensor")
    A = n // B
    _, nproj, rows, C = grads.shape
    R = rows // n
    f32, bf16 = jnp.float32, jnp.bfloat16
    dma = pltpu.SemaphoreType.DMA
    vmem = pl.BlockSpec(memory_space=pltpu.VMEM)
    hbm = pl.BlockSpec(memory_space=pl.ANY)
    block = (nproj, R, C)
    inner = max(B - 1, 1)
    params, new_master, new_moment, new_v = pl.pallas_call(
        functools.partial(kernel, A, B, T, rows),
        name="adam_mini",
        out_shape=[
            jax.ShapeDtypeStruct((nproj, n, R, C), bf16),
            jax.ShapeDtypeStruct(block, f32),
            jax.ShapeDtypeStruct(block, f32),
            jax.ShapeDtypeStruct((nproj, C), f32),
        ],
        in_specs=[hbm, hbm, hbm, pl.BlockSpec(memory_space=pltpu.SMEM), vmem],
        out_specs=[vmem] * 4,
        scratch_shapes=[
            pltpu.VMEM((A, *block), bf16),
            pltpu.VMEM((A, inner, *block), bf16),
            pltpu.VMEM((A, *block), bf16),
            pltpu.VMEM((A, *block), bf16),
            pltpu.VMEM((A, *block), bf16),
            pltpu.VMEM(block, f32),
            pltpu.VMEM(block, f32),
            pltpu.VMEM(block, f32),
            pltpu.VMEM((nproj, C), f32),
            pltpu.VMEM((n - 1, nproj, C), f32),
            pltpu.VMEM((8, HEAD), f32),
            pltpu.VMEM((T - 1, 8, HEAD), f32),
            dma((A, nproj)), dma((2,)),
            dma((A, inner, nproj)), dma((A, inner, nproj)),
            dma((A, nproj)), dma((A, nproj)), dma((A, nproj)),
            dma((n - 1,)), dma((n - 1,)), dma((T - 1,)), dma((T - 1,)),
            dma((A, nproj)), dma((A, nproj)), dma((A, nproj)), dma((A, nproj)),
            dma((A, inner, nproj)), dma((A, inner, nproj)),
        ],
        compiler_params=pltpu.CompilerParams(
            collective_id=0, has_side_effects=True, vmem_limit_bytes=48 * 2**20
        ),
    )(grads.reshape(nproj, n, R, C), master, moment, v_heads, v_neurons.reshape(1, C))
    new_heads = new_v[0].reshape(-1, HEAD)[:, 0]
    return (params.reshape(nproj, rows, C), new_master, new_moment, new_heads, new_v[1])


def solution(mesh):
    in_specs = (
        P("dp", None, None, "tensor"),
        P(None, "dp", "tensor"),
        P(None, "dp", "tensor"),
        P("tensor"),
        P("tensor"),
    )
    out_specs = (
        P(None, None, "tensor"),
        P(None, "dp", "tensor"),
        P(None, "dp", "tensor"),
        P("tensor"),
        P("tensor"),
    )
    return jax.shard_map(
        functools.partial(on_device, inner_size(mesh)),
        mesh=mesh, in_specs=in_specs, out_specs=out_specs, check_vma=False,
    )
```

```python
import functools

import jax
import jax.numpy as jnp
from jax import lax
from jax.experimental import pallas as pl
from jax.experimental.pallas import tpu as pltpu
from jax.sharding import PartitionSpec as P

HEAD = 128
STEP = 2
LIMIT = 480.0
MESH = pl.DeviceIdType.MESH
TILE = 32
KERNEL_LIMIT = 40 * 2**20
WRITER_LIMIT = 16 * 2**20


def encode(x, scale):
    z = x * scale
    return (z * jnp.abs(z) * (z * z)).astype(jnp.bfloat16)


def decode(code, scale):
    y = code.astype(jnp.float32)
    root = lax.rsqrt(lax.rsqrt(jnp.abs(y))) * (1.0 / scale)
    return jnp.where(y < 0, -root, root)


def kernel(
    A, B, T, n_rows,
    grads, master, moment, v_heads, v_neurons,
    params, new_master, new_moment, new_v,
    own, raw, xown, xin, xout, part_out, up_in, down_in, gsum, mas, mom, stat, stat_in, tot, tot_in,
    own_sem, mm_sem, raw_s, raw_r, part_s, up_r, down_r, stat_s, stat_r, tot_s, tot_r,
    zup_s, zup_r, zdn_s, zdn_r, in_s, in_r, xown_sem, xin_s, xin_r, xg_s, xg_r,
):
    nproj, n, R, C = grads.shape
    me = lax.axis_index("dp")
    mt = lax.axis_index("tensor")
    a, b = me // B, me % B
    tile = min(TILE, R)
    scale = 2.0**31 / (LIMIT * n)
    balanced = A >= 4 and B >= 2
    last = nproj - 1
    mated = jnp.logical_or(a <= 1, a >= A - 2) if balanced else jnp.bool_(False)
    mate = jnp.where(a <= 1, 1 - a, 2 * A - 3 - a) if balanced else a

    def unless_mate(at, p, use):
        if balanced and p == last:
            pl.when(jnp.logical_not(jnp.logical_and(mated, at == mate)))(use)
        else:
            use()

    def at_dp(i):
        return {"dp": i}

    def peer(j):
        return (b + j) % B

    barrier = pltpu.get_barrier_semaphore()
    for j in range(1, n):
        pl.semaphore_signal(barrier, inc=1, device_id=at_dp((me + j) % n), device_id_type=MESH)
    for j in range(1, T):
        pl.semaphore_signal(barrier, inc=1, device_id={"tensor": (mt + j) % T}, device_id_type=MESH)

    def own_copy(at, p):
        return pltpu.make_async_copy(grads.at[p, at * B + b], own.at[at, p], own_sem.at[at, p])

    mm = [
        pltpu.make_async_copy(master, mas, mm_sem.at[0]),
        pltpu.make_async_copy(moment, mom, mm_sem.at[1]),
    ]

    def in_order(use, after=None):
        for d in range(A - 1, 0, -1):
            @pl.when(a + d <= A - 1)
            def _():
                use(a + d, 1, d)

            @pl.when(a - d >= 0)
            def _():
                use(a - d, -1, d)
            if after is not None and d == A - 1:
                after()
        use(a, 0, 0)

    def raw_copy(at, j, p):
        to = peer(j)
        return pltpu.make_async_remote_copy(
            src_ref=grads.at[p, at * B + to], dst_ref=raw.at[at, j - 1, p],
            send_sem=raw_s.at[at, j - 1, p], recv_sem=raw_r.at[at, j - 1, p],
            device_id=at_dp(a * B + to), device_id_type=MESH,
        )

    def start_own(at, side, d):
        for p in range(nproj):
            own_copy(at, p).start()

    def start_raw(at, side, d):
        for p in range(nproj):
            def go(p=p):
                for j in range(1, B):
                    raw_copy(at, j, p).start()
            if balanced and p == last and d <= 1:
                skip = mated if side == 0 else jnp.logical_and(mated, at == mate)
                pl.when(jnp.logical_not(skip))(go)
            else:
                go()

    def mate_raw(j):
        return pltpu.make_async_remote_copy(
            src_ref=grads.at[last, mate * B + peer(j)], dst_ref=xin.at[j - 1],
            send_sem=xin_s.at[j - 1], recv_sem=xin_r.at[j - 1],
            device_id=at_dp(mate * B + b), device_id_type=MESH,
        )

    def mate_own(j):
        return pltpu.make_async_copy(grads.at[last, a * B + peer(j)], xown.at[j - 1], xown_sem.at[j - 1])

    def mate_sum(j):
        return pltpu.make_async_remote_copy(
            src_ref=xout.at[j - 1], dst_ref=raw.at[a, j - 1, last],
            send_sem=raw_s.at[a, j - 1, last], recv_sem=raw_r.at[a, j - 1, last],
            device_id=at_dp(a * B + peer(j)), device_id_type=MESH,
        )

    in_order(start_own)
    if balanced:
        @pl.when(mated)
        def _():
            for j in range(1, B):
                mate_own(j).start()
    for c in mm:
        c.start()
    pl.semaphore_wait(barrier, n - 1 + T - 1)
    if balanced:
        @pl.when(mated)
        def _():
            for j in range(1, B):
                mate_raw(j).start()
    in_order(start_raw)

    def up_copy(at, p):
        return pltpu.make_async_remote_copy(
            src_ref=part_out.at[at, p], dst_ref=up_in.at[at, p],
            send_sem=part_s.at[at, p], recv_sem=up_r.at[at, p],
            device_id=at_dp(jnp.minimum(me + B, n - 1)), device_id_type=MESH,
        )

    def down_copy(at, p):
        return pltpu.make_async_remote_copy(
            src_ref=part_out.at[at, p], dst_ref=down_in.at[at, p],
            send_sem=part_s.at[at, p], recv_sem=down_r.at[at, p],
            device_id=at_dp(jnp.maximum(me - B, 0)), device_id_type=MESH,
        )

    def local_sum(at, p, rows, kind="raw"):
        x = own[at, p, rows].astype(jnp.float32)
        for j in range(B - 1 if kind != "own" else 0):
            y = raw[at, j, p, rows]
            x = x + (decode(y, scale) if kind == "coded" else y.astype(jnp.float32))
        return x

    def send_mate_sums():
        @pl.when(mated)
        def _():
            for j in range(1, B):
                mate_own(j).wait()
                mate_raw(j).wait_recv()

                def put(rows, j=j):
                    x = xown[j - 1, rows].astype(jnp.float32) + xin[j - 1, rows].astype(jnp.float32)
                    xout[j - 1, rows] = encode(x, scale)
                tiles(put)
                mate_sum(j).start()

    def tiles(body):
        def step(i, carry):
            body(pl.ds(pl.multiple_of(i * tile, tile), tile))
            return carry
        lax.fori_loop(0, R // tile, step, 0)

    def combine(at, side, d):
        for p in range(nproj):
            if balanced and p == last and d <= 1:
                odd = mated if side == 0 else jnp.logical_and(mated, at == mate)
                pl.when(odd)(functools.partial(combine_one, at, side, p, "coded" if side == 0 else "own"))
                pl.when(jnp.logical_not(odd))(functools.partial(combine_one, at, side, p, "raw"))
            else:
                combine_one(at, side, p, "raw")

    def combine_one(at, side, p, kind):
        own_copy(at, p).wait()
        if kind != "own":
            for j in range(1, B):
                raw_copy(at, j, p).wait_recv()
        if side == 0:
            def begin(rows):
                gsum[p, rows] = local_sum(at, p, rows, kind)
            tiles(begin)
            for inn, copy, cond in ((up_in, up_copy, a > 0), (down_in, down_copy, a < A - 1)):
                @pl.when(cond)
                def _():
                    copy(at, p).wait_recv()

                    def add(rows):
                        gsum[p, rows] = gsum[p, rows] + decode(inn[at, p, rows], scale)
                    tiles(add)
            return
        inn, copy = (up_in, up_copy) if side > 0 else (down_in, down_copy)
        first = (a == 0) if side > 0 else (a == A - 1)

        @pl.when(first)
        def _():
            def put(rows):
                part_out[at, p, rows] = encode(local_sum(at, p, rows, kind), scale)
            tiles(put)

        @pl.when(jnp.logical_not(first))
        def _():
            copy(at, p).wait_recv()

            def put(rows):
                x = local_sum(at, p, rows, kind) + decode(inn[at, p, rows], scale)
                part_out[at, p, rows] = encode(x, scale)
            tiles(put)
        copy(at, p).start()

    in_order(combine, send_mate_sums if balanced else None)

    inv = 1.0 / n

    for p in range(nproj):
        def sq(i, acc):
            rows = pl.ds(pl.multiple_of(i * tile, tile), tile)
            g = gsum[p, rows] * inv
            gsum[p, rows] = g
            g = (g * g).reshape(tile // 8, 8, C)
            return acc + jnp.sum(g, axis=0)
        acc = lax.fori_loop(0, R // tile, sq, jnp.zeros((8, C), jnp.float32))
        stat[p : p + 1, :] = jnp.sum(acc, axis=0, keepdims=True)

    def stat_copy(j):
        return pltpu.make_async_remote_copy(
            src_ref=stat, dst_ref=stat_in.at[j - 1], send_sem=stat_s.at[j - 1], recv_sem=stat_r.at[j - 1],
            device_id=at_dp((me + j) % n), device_id_type=MESH,
        )

    for j in range(1, n):
        stat_copy(j).start()
    sums = stat[...]
    for j in range(1, n):
        stat_copy(j).wait_recv()
        sums = sums + stat_in[j - 1]
    tot[...] = jnp.broadcast_to(jnp.sum(sums), tot.shape)

    def tot_copy(j):
        return pltpu.make_async_remote_copy(
            src_ref=tot, dst_ref=tot_in.at[j - 1], send_sem=tot_s.at[j - 1], recv_sem=tot_r.at[j - 1],
            device_id={"tensor": (mt + j) % T}, device_id_type=MESH,
        )

    for j in range(1, T):
        tot_copy(j).start()
    total = tot[0:1, :]
    for j in range(1, T):
        tot_copy(j).wait_recv()
        total = total + tot_in[j - 1, 0:1, :]
    clip = jnp.minimum(1.0, 256.0 / (jnp.sqrt(total) + 1e-06))
    clip = jnp.concatenate([clip] * (C // HEAD), axis=1)
    heads = []
    for h in range(C // HEAD):
        head = jnp.sum(sums[0:1, h * HEAD : (h + 1) * HEAD], axis=1, keepdims=True)
        heads.append(0.95 * v_heads[h] + 0.05 * (clip * clip)[:, :HEAD] * head / (n_rows * HEAD))
    v_key = jnp.concatenate(heads, axis=1)
    v_val = 0.95 * v_neurons[...] + 0.05 * clip * clip * sums[1:2, :] / n_rows
    new_v[0:1, :] = v_key
    new_v[1:2, :] = v_val
    second_fix = 1.0 - 0.95**STEP
    first_fix = 1.0 - 0.9**STEP
    for c in mm:
        c.wait()

    def up_gather(at, p):
        return pltpu.make_async_remote_copy(
            src_ref=params.at[p, at * B + b], dst_ref=params.at[p, at * B + b],
            send_sem=zup_s.at[at, p], recv_sem=zup_r.at[at, p],
            device_id=at_dp(jnp.minimum(me + B, n - 1)), device_id_type=MESH,
        )

    def down_gather(at, p):
        return pltpu.make_async_remote_copy(
            src_ref=params.at[p, at * B + b], dst_ref=params.at[p, at * B + b],
            send_sem=zdn_s.at[at, p], recv_sem=zdn_r.at[at, p],
            device_id=at_dp(jnp.maximum(me - B, 0)), device_id_type=MESH,
        )

    def in_gather(at, j, p, col):
        return pltpu.make_async_remote_copy(
            src_ref=params.at[p, at * B + col], dst_ref=params.at[p, at * B + col],
            send_sem=in_s.at[at, j - 1, p], recv_sem=in_r.at[at, j - 1, p],
            device_id=at_dp(a * B + peer(j)), device_id_type=MESH,
        )

    def column_from(j):
        return (b - j + B) % B

    def mate_gather(at, j):
        block = params.at[last, at * B + column_from(j)]
        return pltpu.make_async_remote_copy(
            src_ref=block, dst_ref=block, send_sem=xg_s.at[j - 1], recv_sem=xg_r.at[j - 1],
            device_id=at_dp(mate * B + b), device_id_type=MESH,
        )

    for p in range(nproj):
        v = v_key if p == 0 else v_val
        rate = 1.0 / (first_fix * (jnp.sqrt(v / second_fix) + 1e-08))
        gain = 0.1 * clip

        def update(rows):
            fresh = 0.9 * mom[p, rows] + gain * gsum[p, rows]
            w = mas[p, rows]
            w = w - 0.01 * (fresh * rate + 0.1 * w)
            new_moment[p, rows] = fresh
            new_master[p, rows] = w
            params[p, me, rows] = w.astype(jnp.bfloat16)
        tiles(update)
        for j in range(1, B):
            in_gather(a, j, p, b).start()

        @pl.when(a < A - 1)
        def _():
            up_gather(a, p).start()

        @pl.when(a > 0)
        def _():
            down_gather(a, p).start()

    for d in range(1, A):
        for p in range(nproj):
            @pl.when(a - d >= 0)
            def _():
                at = a - d
                up_gather(at, p).wait_recv()

                @pl.when(a < A - 1)
                def _():
                    up_gather(at, p).start()

                def across():
                    for j in range(1, B):
                        in_gather(at, j, p, b).start()
                unless_mate(at, p, across)

            @pl.when(a + d <= A - 1)
            def _():
                at = a + d
                down_gather(at, p).wait_recv()

                @pl.when(a > 0)
                def _():
                    down_gather(at, p).start()

                def across():
                    for j in range(1, B):
                        in_gather(at, j, p, b).start()
                unless_mate(at, p, across)
        if balanced and d == 2:
            @pl.when(mated)
            def _():
                for j in range(1, B):
                    in_gather(a, j, last, column_from(j)).wait_recv()
                    mate_gather(a, j).start()

    def finish(at, side, d):
        for p in range(nproj):
            def across(p=p):
                for j in range(1, B):
                    raw_copy(at, j, p).wait_send()
                    in_gather(at, j, p, b).wait_send()

            def arrive(p=p):
                for j in range(1, B):
                    in_gather(at, j, p, column_from(j)).wait_recv()
            if side == 0:
                across()
                if balanced and p == last:
                    pl.when(jnp.logical_not(mated))(arrive)
                else:
                    arrive()
            else:
                unless_mate(at, p, across)
                unless_mate(at, p, arrive)
            if side > 0:
                up_copy(at, p).wait_send()
            elif side < 0:
                down_copy(at, p).wait_send()
            if side <= 0:
                @pl.when(a < A - 1)
                def _():
                    up_gather(at, p).wait_send()
            if side >= 0:
                @pl.when(a > 0)
                def _():
                    down_gather(at, p).wait_send()

    in_order(finish)
    if balanced:
        @pl.when(mated)
        def _():
            for j in range(1, B):
                mate_raw(j).wait_send()
                mate_gather(a, j).wait_send()
                mate_gather(mate, j).wait_recv()
    for j in range(1, n):
        stat_copy(j).wait_send()
    for j in range(1, T):
        tot_copy(j).wait_send()


def writer(params, new_master, new_moment, new_v, params_out, master_out, moment_out, heads, neurons, sem):
    copies = [
        pltpu.make_async_copy(src, dst, sem.at[i])
        for i, (src, dst) in enumerate(
            ((params, params_out), (new_master, master_out), (new_moment, moment_out))
        )
    ]
    for c in copies:
        c.start()
    for h in range(heads.shape[0]):
        heads[h] = jnp.max(new_v[0:1, h * HEAD : (h + 1) * HEAD])
    neurons[...] = new_v[1:2, :]
    for c in copies:
        c.wait()


def inner_size(mesh):
    line = mesh.devices.reshape(mesh.shape["dp"], -1)[:, 0]
    n = len(line)
    spots = [getattr(d, "coords", None) for d in line]
    if any(s is None or len(s) < 3 for s in spots):
        return 2 if n % 2 == 0 else 1
    inner = sum(s[2] == spots[0][2] for s in spots)
    return inner if n % inner == 0 else 1


def on_device(B, grads, master, moment, v_heads, v_neurons):
    n, T = lax.axis_size("dp"), lax.axis_size("tensor")
    A = n // B
    _, nproj, rows, C = grads.shape
    R = rows // n
    f32, bf16 = jnp.float32, jnp.bfloat16
    dma = pltpu.SemaphoreType.DMA
    vmem = pl.BlockSpec(memory_space=pltpu.VMEM)
    hbm = pl.BlockSpec(memory_space=pltpu.HBM)
    block = (nproj, R, C)
    inner = max(B - 1, 1)
    params, new_master, new_moment, new_v = pl.pallas_call(
        functools.partial(kernel, A, B, T, rows),
        name="adam_mini",
        out_shape=[
            jax.ShapeDtypeStruct((nproj, n, R, C), bf16),
            jax.ShapeDtypeStruct(block, f32),
            jax.ShapeDtypeStruct(block, f32),
            jax.ShapeDtypeStruct((nproj, C), f32),
        ],
        in_specs=[hbm, hbm, hbm, pl.BlockSpec(memory_space=pltpu.SMEM), vmem],
        out_specs=[vmem] * 4,
        scratch_shapes=[
            pltpu.VMEM((A, *block), bf16),
            pltpu.VMEM((A, inner, *block), bf16),
            pltpu.VMEM((inner, R, C), bf16),
            pltpu.VMEM((inner, R, C), bf16),
            pltpu.VMEM((inner, R, C), bf16),
            pltpu.VMEM((A, *block), bf16),
            pltpu.VMEM((A, *block), bf16),
            pltpu.VMEM((A, *block), bf16),
            pltpu.VMEM(block, f32),
            pltpu.VMEM(block, f32),
            pltpu.VMEM(block, f32),
            pltpu.VMEM((nproj, C), f32),
            pltpu.VMEM((n - 1, nproj, C), f32),
            pltpu.VMEM((8, HEAD), f32),
            pltpu.VMEM((T - 1, 8, HEAD), f32),
            dma((A, nproj)), dma((2,)),
            dma((A, inner, nproj)), dma((A, inner, nproj)),
            dma((A, nproj)), dma((A, nproj)), dma((A, nproj)),
            dma((n - 1,)), dma((n - 1,)), dma((T - 1,)), dma((T - 1,)),
            dma((A, nproj)), dma((A, nproj)), dma((A, nproj)), dma((A, nproj)),
            dma((A, inner, nproj)), dma((A, inner, nproj)),
            dma((inner,)), dma((inner,)), dma((inner,)), dma((inner,)), dma((inner,)),
        ],
        compiler_params=pltpu.CompilerParams(
            collective_id=0, has_side_effects=True, vmem_limit_bytes=KERNEL_LIMIT
        ),
    )(grads.reshape(nproj, n, R, C), master, moment, v_heads, v_neurons.reshape(1, C))
    heads = v_heads.shape[0]
    params, new_master, new_moment, new_heads, new_neurons = pl.pallas_call(
        writer,
        name="write_out",
        out_shape=[
            jax.ShapeDtypeStruct((nproj, n, R, C), bf16),
            jax.ShapeDtypeStruct(block, f32),
            jax.ShapeDtypeStruct(block, f32),
            jax.ShapeDtypeStruct((heads,), f32),
            jax.ShapeDtypeStruct((1, C), f32),
        ],
        in_specs=[vmem] * 4,
        out_specs=[pl.BlockSpec(memory_space=pltpu.HBM)] * 3 + [pl.BlockSpec(memory_space=pltpu.SMEM), vmem],
        scratch_shapes=[dma((3,))],
        compiler_params=pltpu.CompilerParams(vmem_limit_bytes=WRITER_LIMIT),
    )(params, new_master, new_moment, new_v)
    return (
        params.reshape(nproj, rows, C), new_master, new_moment, new_heads, new_neurons.reshape(C),
    )


def solution(mesh):
    in_specs = (
        P("dp", None, None, "tensor"),
        P(None, "dp", "tensor"),
        P(None, "dp", "tensor"),
        P("tensor"),
        P("tensor"),
    )
    out_specs = (
        P(None, None, "tensor"),
        P(None, "dp", "tensor"),
        P(None, "dp", "tensor"),
        P("tensor"),
        P("tensor"),
    )
    return jax.shard_map(
        functools.partial(on_device, inner_size(mesh)),
        mesh=mesh, in_specs=in_specs, out_specs=out_specs, check_vma=False,
    )
```

```python
import functools

import jax
import jax.numpy as jnp
from jax import lax
from jax.experimental import pallas as pl
from jax.experimental.pallas import tpu as pltpu
from jax.sharding import PartitionSpec as P

HEAD = 128
STEP = 2
LIMIT = 480.0
MESH = pl.DeviceIdType.MESH
TILE = 32
KERNEL_LIMIT = 43 * 2**20
WRITER_LIMIT = 16 * 2**20


def encode(x, scale):
    z = x * scale
    return (z * jnp.abs(z) * (z * z)).astype(jnp.bfloat16)


def decode(code, scale):
    y = code.astype(jnp.float32)
    root = lax.rsqrt(lax.rsqrt(jnp.abs(y))) * (1.0 / scale)
    return jnp.where(y < 0, -root, root)


def kernel(
    A, B, T, n_rows,
    grads, master, moment, v_heads, v_neurons,
    params, new_master, new_moment, new_v,
    own, raw, xown, xin, xout, part_out, up_in, down_in, gsum, mas, mom, stat, stat_in, tot, tot_in,
    own_sem, mm_sem, raw_s, raw_r, part_s, up_r, down_r, stat_s, stat_r, tot_s, tot_r,
    zup_s, zup_r, zdn_s, zdn_r, in_s, in_r, xown_sem, xin_s, xin_r, xup_s, xup_r, xdn_s, xdn_r,
):
    nproj, n, R, C = grads.shape
    me = lax.axis_index("dp")
    mt = lax.axis_index("tensor")
    a, b = me // B, me % B
    tile = min(TILE, R)
    scale = 2.0**31 / (LIMIT * n)
    balanced = A >= 4 and B >= 2
    last = nproj - 1
    mated = jnp.logical_or(a <= 1, a >= A - 2) if balanced else jnp.bool_(False)
    mate = jnp.where(a <= 1, 1 - a, 2 * A - 3 - a) if balanced else a

    def unless_mate(at, p, use):
        if balanced and p == last:
            pl.when(jnp.logical_not(jnp.logical_and(mated, at == mate)))(use)
        else:
            use()

    def at_dp(i):
        return {"dp": i}

    def peer(j):
        return (b + j) % B

    barrier = pltpu.get_barrier_semaphore()
    for j in range(1, n):
        pl.semaphore_signal(barrier, inc=1, device_id=at_dp((me + j) % n), device_id_type=MESH)
    for j in range(1, T):
        pl.semaphore_signal(barrier, inc=1, device_id={"tensor": (mt + j) % T}, device_id_type=MESH)

    def own_copy(at, p):
        return pltpu.make_async_copy(grads.at[p, at * B + b], own.at[at, p], own_sem.at[at, p])

    mm = [
        pltpu.make_async_copy(master, mas, mm_sem.at[0]),
        pltpu.make_async_copy(moment, mom, mm_sem.at[1]),
    ]

    def in_order(use, after=None):
        for d in range(A - 1, 0, -1):
            @pl.when(a + d <= A - 1)
            def _():
                use(a + d, 1, d)

            @pl.when(a - d >= 0)
            def _():
                use(a - d, -1, d)
            if after is not None and d == A - 1:
                after()
        use(a, 0, 0)

    def raw_copy(at, j, p):
        to = peer(j)
        return pltpu.make_async_remote_copy(
            src_ref=grads.at[p, at * B + to], dst_ref=raw.at[at, j - 1, p],
            send_sem=raw_s.at[at, j - 1, p], recv_sem=raw_r.at[at, j - 1, p],
            device_id=at_dp(a * B + to), device_id_type=MESH,
        )

    def start_own(at, side, d):
        for p in range(nproj):
            own_copy(at, p).start()

    def start_raw(at, side, d):
        for p in range(nproj):
            def go(p=p):
                for j in range(1, B):
                    raw_copy(at, j, p).start()
            if balanced and p == last and d <= 1:
                skip = mated if side == 0 else jnp.logical_and(mated, at == mate)
                pl.when(jnp.logical_not(skip))(go)
            else:
                go()

    def mate_raw(j):
        return pltpu.make_async_remote_copy(
            src_ref=grads.at[last, mate * B + peer(j)], dst_ref=xin.at[j - 1],
            send_sem=xin_s.at[j - 1], recv_sem=xin_r.at[j - 1],
            device_id=at_dp(mate * B + b), device_id_type=MESH,
        )

    def mate_own(j):
        return pltpu.make_async_copy(grads.at[last, a * B + peer(j)], xown.at[j - 1], xown_sem.at[j - 1])

    def mate_sum(j):
        return pltpu.make_async_remote_copy(
            src_ref=xout.at[j - 1], dst_ref=raw.at[a, j - 1, last],
            send_sem=raw_s.at[a, j - 1, last], recv_sem=raw_r.at[a, j - 1, last],
            device_id=at_dp(a * B + peer(j)), device_id_type=MESH,
        )

    in_order(start_own)
    if balanced:
        @pl.when(mated)
        def _():
            for j in range(1, B):
                mate_own(j).start()
    for c in mm:
        c.start()
    pl.semaphore_wait(barrier, n - 1 + T - 1)
    if balanced:
        @pl.when(mated)
        def _():
            for j in range(1, B):
                mate_raw(j).start()
    in_order(start_raw)

    def up_copy(at, p):
        return pltpu.make_async_remote_copy(
            src_ref=part_out.at[at, p], dst_ref=up_in.at[at, p],
            send_sem=part_s.at[at, p], recv_sem=up_r.at[at, p],
            device_id=at_dp(jnp.minimum(me + B, n - 1)), device_id_type=MESH,
        )

    def down_copy(at, p):
        return pltpu.make_async_remote_copy(
            src_ref=part_out.at[at, p], dst_ref=down_in.at[at, p],
            send_sem=part_s.at[at, p], recv_sem=down_r.at[at, p],
            device_id=at_dp(jnp.maximum(me - B, 0)), device_id_type=MESH,
        )

    def local_sum(at, p, rows, kind="raw"):
        x = own[at, p, rows].astype(jnp.float32)
        for j in range(B - 1 if kind != "own" else 0):
            y = raw[at, j, p, rows]
            x = x + (decode(y, scale) if kind == "coded" else y.astype(jnp.float32))
        return x

    def send_mate_sums():
        @pl.when(mated)
        def _():
            for j in range(1, B):
                mate_own(j).wait()
                mate_raw(j).wait_recv()

                def put(rows, j=j):
                    x = xown[j - 1, rows].astype(jnp.float32) + xin[j - 1, rows].astype(jnp.float32)
                    xout[j - 1, rows] = encode(x, scale)
                tiles(put)
                mate_sum(j).start()

    def tiles(body):
        def step(i, carry):
            body(pl.ds(pl.multiple_of(i * tile, tile), tile))
            return carry
        lax.fori_loop(0, R // tile, step, 0)

    def combine(at, side, d):
        for p in range(nproj):
            if balanced and p == last and d <= 1:
                odd = mated if side == 0 else jnp.logical_and(mated, at == mate)
                pl.when(odd)(functools.partial(combine_one, at, side, p, "coded" if side == 0 else "own"))
                pl.when(jnp.logical_not(odd))(functools.partial(combine_one, at, side, p, "raw"))
            else:
                combine_one(at, side, p, "raw")

    def combine_one(at, side, p, kind):
        own_copy(at, p).wait()
        if kind != "own":
            for j in range(1, B):
                raw_copy(at, j, p).wait_recv()
        if side == 0:
            def close(up, down):
                for used, inn, copy in ((up, up_in, up_copy), (down, down_in, down_copy)):
                    if used:
                        copy(at, p).wait_recv()

                def one(i, acc):
                    rows = pl.ds(pl.multiple_of(i * tile, tile), tile)
                    g = local_sum(at, p, rows, kind)
                    if up:
                        g = g + decode(up_in[at, p, rows], scale)
                    if down:
                        g = g + decode(down_in[at, p, rows], scale)
                    g = g * (1.0 / n)
                    gsum[p, rows] = g
                    return acc + jnp.sum((g * g).reshape(tile // 8, 8, C), axis=0)
                acc = lax.fori_loop(0, R // tile, one, jnp.zeros((8, C), jnp.float32))
                stat[p : p + 1, :] = jnp.sum(acc, axis=0, keepdims=True)

            if A == 1:
                close(False, False)
            else:
                pl.when(a == 0)(lambda: close(False, True))
                pl.when(a == A - 1)(lambda: close(True, False))
                pl.when(jnp.logical_and(a > 0, a < A - 1))(lambda: close(True, True))
            return
        inn, copy = (up_in, up_copy) if side > 0 else (down_in, down_copy)
        first = (a == 0) if side > 0 else (a == A - 1)

        @pl.when(first)
        def _():
            def put(rows):
                part_out[at, p, rows] = encode(local_sum(at, p, rows, kind), scale)
            tiles(put)

        @pl.when(jnp.logical_not(first))
        def _():
            copy(at, p).wait_recv()

            def put(rows):
                x = local_sum(at, p, rows, kind) + decode(inn[at, p, rows], scale)
                part_out[at, p, rows] = encode(x, scale)
            tiles(put)
        copy(at, p).start()

    in_order(combine, send_mate_sums if balanced else None)

    def stat_copy(j):
        return pltpu.make_async_remote_copy(
            src_ref=stat, dst_ref=stat_in.at[j - 1], send_sem=stat_s.at[j - 1], recv_sem=stat_r.at[j - 1],
            device_id=at_dp((me + j) % n), device_id_type=MESH,
        )

    for j in range(1, n):
        stat_copy(j).start()
    sums = stat[...]
    for j in range(1, n):
        stat_copy(j).wait_recv()
        sums = sums + stat_in[j - 1]
    tot[...] = jnp.broadcast_to(jnp.sum(sums), tot.shape)

    def tot_copy(j):
        return pltpu.make_async_remote_copy(
            src_ref=tot, dst_ref=tot_in.at[j - 1], send_sem=tot_s.at[j - 1], recv_sem=tot_r.at[j - 1],
            device_id={"tensor": (mt + j) % T}, device_id_type=MESH,
        )

    for j in range(1, T):
        tot_copy(j).start()
    total = tot[0:1, :]
    for j in range(1, T):
        tot_copy(j).wait_recv()
        total = total + tot_in[j - 1, 0:1, :]
    clip = jnp.minimum(1.0, 256.0 / (jnp.sqrt(total) + 1e-06))
    clip = jnp.concatenate([clip] * (C // HEAD), axis=1)
    heads = []
    for h in range(C // HEAD):
        head = jnp.sum(sums[0:1, h * HEAD : (h + 1) * HEAD], axis=1, keepdims=True)
        heads.append(0.95 * v_heads[h] + 0.05 * (clip * clip)[:, :HEAD] * head / (n_rows * HEAD))
    v_key = jnp.concatenate(heads, axis=1)
    v_val = 0.95 * v_neurons[...] + 0.05 * clip * clip * sums[1:2, :] / n_rows
    new_v[0:1, :] = v_key
    new_v[1:2, :] = v_val
    second_fix = 1.0 - 0.95**STEP
    first_fix = 1.0 - 0.9**STEP
    for c in mm:
        c.wait()

    def up_gather(at, p):
        return pltpu.make_async_remote_copy(
            src_ref=params.at[p, at * B + b], dst_ref=params.at[p, at * B + b],
            send_sem=zup_s.at[at, p], recv_sem=zup_r.at[at, p],
            device_id=at_dp(jnp.minimum(me + B, n - 1)), device_id_type=MESH,
        )

    def down_gather(at, p):
        return pltpu.make_async_remote_copy(
            src_ref=params.at[p, at * B + b], dst_ref=params.at[p, at * B + b],
            send_sem=zdn_s.at[at, p], recv_sem=zdn_r.at[at, p],
            device_id=at_dp(jnp.maximum(me - B, 0)), device_id_type=MESH,
        )

    def in_gather(at, j, p, col):
        return pltpu.make_async_remote_copy(
            src_ref=params.at[p, at * B + col], dst_ref=params.at[p, at * B + col],
            send_sem=in_s.at[at, j - 1, p], recv_sem=in_r.at[at, j - 1, p],
            device_id=at_dp(a * B + peer(j)), device_id_type=MESH,
        )

    def column_from(j):
        return (b - j + B) % B

    def x_up(j):
        block = params.at[last, column_from(j)]
        return pltpu.make_async_remote_copy(
            src_ref=block, dst_ref=block, send_sem=xup_s.at[j - 1], recv_sem=xup_r.at[j - 1],
            device_id=at_dp(jnp.minimum(me + B, n - 1)), device_id_type=MESH,
        )

    def x_down(j):
        block = params.at[last, (A - 1) * B + column_from(j)]
        return pltpu.make_async_remote_copy(
            src_ref=block, dst_ref=block, send_sem=xdn_s.at[j - 1], recv_sem=xdn_r.at[j - 1],
            device_id=at_dp(jnp.maximum(me - B, 0)), device_id_type=MESH,
        )

    def unless_end(at, p, use):
        if balanced and p == last:
            pl.when(jnp.logical_and(at > 0, at < A - 1))(use)
        else:
            use()

    for p in range(nproj):
        v = v_key if p == 0 else v_val
        rate = 1.0 / (first_fix * (jnp.sqrt(v / second_fix) + 1e-08))
        gain = 0.1 * clip

        def update(rows):
            fresh = 0.9 * mom[p, rows] + gain * gsum[p, rows]
            w = mas[p, rows]
            w = w - 0.01 * (fresh * rate + 0.1 * w)
            new_moment[p, rows] = fresh
            new_master[p, rows] = w
            params[p, me, rows] = w.astype(jnp.bfloat16)
        tiles(update)
        for j in range(1, B):
            in_gather(a, j, p, b).start()

        @pl.when(a < A - 1)
        def _():
            up_gather(a, p).start()

        @pl.when(a > 0)
        def _():
            down_gather(a, p).start()

    for d in range(1, A):
        for p in range(nproj):
            @pl.when(a - d >= 0)
            def _():
                at = a - d
                up_gather(at, p).wait_recv()

                @pl.when(a < A - 1)
                def _():
                    up_gather(at, p).start()

                def across():
                    for j in range(1, B):
                        in_gather(at, j, p, b).start()
                unless_end(at, p, across)

            @pl.when(a + d <= A - 1)
            def _():
                at = a + d
                down_gather(at, p).wait_recv()

                @pl.when(a > 0)
                def _():
                    down_gather(at, p).start()

                def across():
                    for j in range(1, B):
                        in_gather(at, j, p, b).start()
                unless_end(at, p, across)
        if balanced:
            for up, near, more, copy in ((True, a == d, a < A - 1, x_up), (False, A - 1 - a == d, a > 0, x_down)):
                @pl.when(near)
                def _():
                    for j in range(1, B):
                        copy(j).wait_recv()

                        @pl.when(more)
                        def _():
                            copy(j).start()
                if d == 1:
                    @pl.when(a == (0 if up else A - 1))
                    def _():
                        for j in range(1, B):
                            in_gather(a, j, last, column_from(j)).wait_recv()
                            copy(j).start()

    def finish(at, side, d):
        for p in range(nproj):
            def raw_sent(p=p):
                for j in range(1, B):
                    raw_copy(at, j, p).wait_send()

            def sent(p=p):
                for j in range(1, B):
                    in_gather(at, j, p, b).wait_send()

            def arrived(p=p):
                for j in range(1, B):
                    in_gather(at, j, p, column_from(j)).wait_recv()
            if side == 0:
                raw_sent()
                sent()
            else:
                unless_mate(at, p, raw_sent)
                unless_end(at, p, sent)
            unless_end(at, p, arrived)
            if side > 0:
                up_copy(at, p).wait_send()
            elif side < 0:
                down_copy(at, p).wait_send()
            if side <= 0:
                @pl.when(a < A - 1)
                def _():
                    up_gather(at, p).wait_send()
            if side >= 0:
                @pl.when(a > 0)
                def _():
                    down_gather(at, p).wait_send()

    in_order(finish)
    if balanced:
        @pl.when(mated)
        def _():
            for j in range(1, B):
                mate_raw(j).wait_send()
        for j in range(1, B):
            pl.when(a < A - 1)(lambda j=j: x_up(j).wait_send())
            pl.when(a > 0)(lambda j=j: x_down(j).wait_send())
    for j in range(1, n):
        stat_copy(j).wait_send()
    for j in range(1, T):
        tot_copy(j).wait_send()


def writer(params, new_master, new_moment, new_v, params_out, master_out, moment_out, heads, neurons, sem):
    copies = [
        pltpu.make_async_copy(src, dst, sem.at[i])
        for i, (src, dst) in enumerate(
            ((params, params_out), (new_master, master_out), (new_moment, moment_out))
        )
    ]
    for c in copies:
        c.start()
    for h in range(heads.shape[0]):
        heads[h] = jnp.max(new_v[0:1, h * HEAD : (h + 1) * HEAD])
    neurons[...] = new_v[1:2, :]
    for c in copies:
        c.wait()


def inner_size(mesh):
    line = mesh.devices.reshape(mesh.shape["dp"], -1)[:, 0]
    n = len(line)
    spots = [getattr(d, "coords", None) for d in line]
    if any(s is None or len(s) < 3 for s in spots):
        return 2 if n % 2 == 0 else 1
    inner = sum(s[2] == spots[0][2] for s in spots)
    return inner if n % inner == 0 else 1


def on_device(B, grads, master, moment, v_heads, v_neurons):
    n, T = lax.axis_size("dp"), lax.axis_size("tensor")
    A = n // B
    _, nproj, rows, C = grads.shape
    R = rows // n
    f32, bf16 = jnp.float32, jnp.bfloat16
    dma = pltpu.SemaphoreType.DMA
    vmem = pl.BlockSpec(memory_space=pltpu.VMEM)
    hbm = pl.BlockSpec(memory_space=pltpu.HBM)
    block = (nproj, R, C)
    inner = max(B - 1, 1)
    params, new_master, new_moment, new_v = pl.pallas_call(
        functools.partial(kernel, A, B, T, rows),
        name="adam_mini",
        out_shape=[
            jax.ShapeDtypeStruct((nproj, n, R, C), bf16),
            jax.ShapeDtypeStruct(block, f32),
            jax.ShapeDtypeStruct(block, f32),
            jax.ShapeDtypeStruct((nproj, C), f32),
        ],
        in_specs=[hbm, hbm, hbm, pl.BlockSpec(memory_space=pltpu.SMEM), vmem],
        out_specs=[vmem] * 4,
        scratch_shapes=[
            pltpu.VMEM((A, *block), bf16),
            pltpu.VMEM((A, inner, *block), bf16),
            pltpu.VMEM((inner, R, C), bf16),
            pltpu.VMEM((inner, R, C), bf16),
            pltpu.VMEM((inner, R, C), bf16),
            pltpu.VMEM((A, *block), bf16),
            pltpu.VMEM((A, *block), bf16),
            pltpu.VMEM((A, *block), bf16),
            pltpu.VMEM(block, f32),
            pltpu.VMEM(block, f32),
            pltpu.VMEM(block, f32),
            pltpu.VMEM((nproj, C), f32),
            pltpu.VMEM((n - 1, nproj, C), f32),
            pltpu.VMEM((8, HEAD), f32),
            pltpu.VMEM((T - 1, 8, HEAD), f32),
            dma((A, nproj)), dma((2,)),
            dma((A, inner, nproj)), dma((A, inner, nproj)),
            dma((A, nproj)), dma((A, nproj)), dma((A, nproj)),
            dma((n - 1,)), dma((n - 1,)), dma((T - 1,)), dma((T - 1,)),
            dma((A, nproj)), dma((A, nproj)), dma((A, nproj)), dma((A, nproj)),
            dma((A, inner, nproj)), dma((A, inner, nproj)),
            dma((inner,)), dma((inner,)), dma((inner,)),
            dma((inner,)), dma((inner,)), dma((inner,)), dma((inner,)),
        ],
        compiler_params=pltpu.CompilerParams(
            collective_id=0, has_side_effects=True, vmem_limit_bytes=KERNEL_LIMIT
        ),
    )(grads.reshape(nproj, n, R, C), master, moment, v_heads, v_neurons.reshape(1, C))
    heads = v_heads.shape[0]
    params, new_master, new_moment, new_heads, new_neurons = pl.pallas_call(
        writer,
        name="write_out",
        out_shape=[
            jax.ShapeDtypeStruct((nproj, n, R, C), bf16),
            jax.ShapeDtypeStruct(block, f32),
            jax.ShapeDtypeStruct(block, f32),
            jax.ShapeDtypeStruct((heads,), f32),
            jax.ShapeDtypeStruct((1, C), f32),
        ],
        in_specs=[vmem] * 4,
        out_specs=[pl.BlockSpec(memory_space=pltpu.HBM)] * 3 + [pl.BlockSpec(memory_space=pltpu.SMEM), vmem],
        scratch_shapes=[dma((3,))],
        compiler_params=pltpu.CompilerParams(vmem_limit_bytes=WRITER_LIMIT),
    )(params, new_master, new_moment, new_v)
    return (
        params.reshape(nproj, rows, C), new_master, new_moment, new_heads, new_neurons.reshape(C),
    )


def solution(mesh):
    in_specs = (
        P("dp", None, None, "tensor"),
        P(None, "dp", "tensor"),
        P(None, "dp", "tensor"),
        P("tensor"),
        P("tensor"),
    )
    out_specs = (
        P(None, None, "tensor"),
        P(None, "dp", "tensor"),
        P(None, "dp", "tensor"),
        P("tensor"),
        P("tensor"),
    )
    return jax.shard_map(
        functools.partial(on_device, inner_size(mesh)),
        mesh=mesh, in_specs=in_specs, out_specs=out_specs, check_vma=False,
    )
```
